16 devices in a mesh: by: 2 (over z), bx: 8 (over y, x, core).
Axes of the slice: x: 2, y: 2, z: 2, core: 2. Of those that a mesh axis runs over, the one named last changes fastest.
Arguments:
- wave_fn: float32 [3072, 2, 2, 3072], P('bx', None, None, 'by')
- left_env: float32 [3072, 3, 3072], P('bx')
- mpo_ten: float32 [3, 2, 2, 3], replicated
- right_env: float32 [3072, 3, 3072], P('by')
Outputs:
- output: float32 [3072, 2, 2, 3072], P('bx', None, None, 'by')
All inputs are finite; a program needn't handle non-finite values.
Results may differ from the reference program's by a relative error of at most 0.001.
Values sent between devices are 32-bit elements.
A program may use at most 1 GiB of HBM per device.

```python
import jax
import jax.numpy as jnp
from jax import lax

BOND_DIM = 3072
PHYS_DIM = 2
MPO_DIM = 3


def setup_inputs(seed: int = 0) -> dict:
    key = jax.random.key(seed)
    k_wave, k_left, k_mpo, k_right = jax.random.split(key, 4)
    wave_fn = jax.random.normal(k_wave, (BOND_DIM, PHYS_DIM, PHYS_DIM, BOND_DIM), jnp.float32)
    left_env = jax.random.normal(k_left, (BOND_DIM, MPO_DIM, BOND_DIM), jnp.float32) * (BOND_DIM ** -0.5)
    mpo_ten = jax.random.normal(k_mpo, (MPO_DIM, PHYS_DIM, PHYS_DIM, MPO_DIM), jnp.float32) * ((MPO_DIM * PHYS_DIM) ** -0.5)
    right_env = jax.random.normal(k_right, (BOND_DIM, MPO_DIM, BOND_DIM), jnp.float32) * ((MPO_DIM * BOND_DIM) ** -0.5)
    return {'wave_fn': wave_fn, 'left_env': left_env, 'mpo_ten': mpo_ten, 'right_env': right_env}


def reference(wave_fn, left_env, mpo_ten, right_env):
    row_block = min(BOND_DIM, 128)
    block_count = BOND_DIM // row_block
    left_blocks = left_env.reshape(block_count, row_block, MPO_DIM, BOND_DIM)

    def one_block(left_rows):
        stage_one = jnp.einsum('auc,cpqf->aupqf', left_rows.astype(jnp.float32), wave_fn.astype(jnp.float32))
        stage_two = jnp.einsum('aupqf,uspv->asvqf', stage_one, mpo_ten.astype(jnp.float32))
        stage_three = jnp.einsum('asvqf,vtqr->astrf', stage_two, mpo_ten.astype(jnp.float32))
        return jnp.einsum('astrf,brf->astb', stage_three, right_env.astype(jnp.float32))

    out_blocks = lax.map(one_block, left_blocks)
    return out_blocks.reshape(BOND_DIM, PHYS_DIM, PHYS_DIM, BOND_DIM)
```

```python
import functools
import jax
import jax.numpy as jnp
from jax import lax
from jax.experimental import pallas as pl
from jax.experimental.pallas import tpu as pltpu
from jax.sharding import PartitionSpec as P

MESH = pl.DeviceIdType.MESH
BF, F32 = jnp.bfloat16, jnp.float32
FB = 256
BT = 512

OWN, XN, YN, DN = 0, 1, 2, 3
UNITS = [(OWN, k) for k in range(6)]
UNITS += [(XN, 0), (YN, 0), (XN, 1), (YN, 1), (DN, 0)]
for _k in range(2, 6):
    UNITS += [(XN, _k), (YN, _k), (DN, _k - 1)]
UNITS += [(DN, 5)]


def split3(v):
    hi = v.astype(BF)
    rest = v - hi.astype(F32)
    mid = rest.astype(BF)
    low = (rest - mid.astype(F32)).astype(BF)
    return hi, mid, low


def dot6(a, b, rhs_dim):
    def d(i, j):
        return lax.dot_general(a[i], b[j], (((1,), (rhs_dim,)), ((), ())), preferred_element_type=F32)
    return d(0, 0) + d(1, 0) + d(2, 0) + d(0, 1) + d(1, 1) + d(0, 2)


def table(i, values):
    out = values[0]
    for k, v in enumerate(values):
        if v != values[0]:
            out = jnp.where(i == k, v, out)
    return out


def kernel(x_ref, l_ref, r_ref, w_ref, y_ref, xg, rx, ys, yr,
           t_ref, xbuf, lbuf, lsp, acc, rbuf, yrbuf,
           ssem, rsem, zsend, zrecv, bsend, brecv, ysend, yrecv, xsem, lsem, bsem, asem, ysem, osem):
    z = lax.axis_index('by')
    me = lax.axis_index('bx')
    core = lax.rem(me, 2)
    cx = lax.rem(me // 2, 2)
    cy = me // 4
    nf = x_ref.shape[3] // FB
    nb = x_ref.shape[3] // BT
    rows = x_ref.shape[0]
    half = rows // 2
    cols = x_ref.shape[3]

    def index(dx, dy, dc):
        return (lax.rem(cy + dy, 2) * 2 + lax.rem(cx + dx, 2)) * 2 + lax.rem(core + dc, 2)

    sib, xn, yn, dn = index(0, 0, 1), index(1, 0, 0), index(0, 1, 0), index(1, 1, 0)
    dev_s, dev_x, dev_y, dev_z = (z, sib), (z, xn), (z, yn), (1 - z, me)

    barrier = pltpu.get_barrier_semaphore()
    for dev in (dev_s, dev_x, dev_y, dev_z):
        pl.semaphore_signal(barrier, inc=1, device_id=dev, device_id_type=MESH)
    pl.semaphore_wait(barrier, 4)

    def piece(ref, k):
        return ref.at[:, :, :, pl.ds(pl.multiple_of(k * FB, FB), FB)]

    def rcopy(src, dst, kind, k, dev):
        return pltpu.make_async_remote_copy(src_ref=src, dst_ref=dst, send_sem=ssem.at[kind, k], recv_sem=rsem.at[kind, k],
                                            device_id=dev, device_id_type=MESH)

    def copy(kind, k):
        if kind == 0:
            return rcopy(piece(x_ref, k), piece(xg.at[me], k), 0, k, dev_s)
        if kind == 1:
            return rcopy(piece(x_ref, k), piece(xg.at[me], k), 1, k, dev_x)
        if kind == 2:
            return rcopy(piece(x_ref, k), piece(xg.at[me], k), 2, k, dev_y)
        if kind == 3:
            part = piece(xg.at[yn, pl.ds(0, half)], k)
            return rcopy(part, part, 3, k, dev_x)
        if kind == 4:
            part = piece(xg.at[xn, pl.ds(half, half)], k)
            return rcopy(part, part, 4, k, dev_y)
        part = piece(xg.at[(xn, yn, dn)[kind - 5]], k)
        return rcopy(part, part, kind, k, dev_s)

    def got(kind, k):
        if kind == 0:
            part = piece(xg.at[sib], k)
        elif kind == 1:
            part = piece(xg.at[xn], k)
        elif kind == 2:
            part = piece(xg.at[yn], k)
        elif kind == 3:
            part = piece(xg.at[dn, pl.ds(0, half)], k)
        elif kind == 4:
            part = piece(xg.at[dn, pl.ds(half, half)], k)
        else:
            part = piece(xg.at[(index(1, 0, 1), index(0, 1, 1), index(1, 1, 1))[kind - 5]], k)
        return rcopy(part, part, kind, k, dev_s)

    hw = cols // 2

    def rz(bt):
        rws = pl.ds(bt * BT, BT)
        src = r_ref.at[:, rws, pl.ds(pl.multiple_of((1 - z) * cols + core * hw, 128), hw)]
        dst = rx.at[:, rws, pl.ds(pl.multiple_of(core * hw, 128), hw)]
        return pltpu.make_async_remote_copy(src_ref=src, dst_ref=dst, send_sem=zsend.at[bt], recv_sem=zrecv.at[bt],
                                            device_id=dev_z, device_id_type=MESH)

    def rs(bt, c):
        part = rx.at[:, pl.ds(bt * BT, BT), pl.ds(pl.multiple_of(c * hw, 128), hw)]
        return pltpu.make_async_remote_copy(src_ref=part, dst_ref=part, send_sem=bsend.at[bt], recv_sem=brecv.at[bt],
                                            device_id=dev_s, device_id_type=MESH)

    def yz(bt):
        return pltpu.make_async_remote_copy(src_ref=ys.at[bt], dst_ref=yr.at[bt], send_sem=ysend.at[bt], recv_sem=yrecv.at[bt],
                                            device_id=dev_z, device_id_type=MESH)

    def own_out(k):
        copy(1, k).start()
        copy(2, k).start()

    def event_xy(k):
        got(1, k).wait_recv()
        copy(4, k).start()
        copy(5, k).start()
        got(2, k).wait_recv()
        copy(3, k).start()
        copy(6, k).start()

    def event_d(k):
        got(3, k).wait_recv()
        got(4, k).wait_recv()
        copy(7, k).start()

    def event_r(bt):
        rz(bt).wait_recv()
        rs(bt, core).start()

    events = {i: [] for i in range(len(UNITS))}
    events[3] += [lambda: event_xy(0), lambda: own_out(2)]
    events[6] += [lambda: event_xy(1), lambda: own_out(3)]
    events[8] += [lambda: event_d(0)]
    for k in range(2, 6):
        i = UNITS.index((XN, k)) - 1
        events[i] += [functools.partial(event_xy, k)]
        if k + 2 < 6:
            events[i] += [functools.partial(own_out, k + 2)]
    for k in range(1, 6):
        i = UNITS.index((DN, k)) - 1
        events[i] += [functools.partial(event_d, k)]
    events[12] += [lambda: event_r(0)]
    events[19] += [lambda: event_r(1)]

    def xload(slot, rel, k):
        px = lax.rem(cx + lax.rem(rel, 2), 2)
        py = lax.rem(cy + rel // 2, 2)
        chip = py * 2 + px
        a = pltpu.make_async_copy(piece(xg.at[chip * 2 + core], k), xbuf.at[slot, core], xsem.at[slot, 0])
        o = pltpu.make_async_copy(piece(x_ref, k), xbuf.at[slot, core], xsem.at[slot, 0])
        b = pltpu.make_async_copy(piece(xg.at[chip * 2 + 1 - core], k), xbuf.at[slot, 1 - core], xsem.at[slot, 1])
        lc = pltpu.make_async_copy(l_ref.at[:, :, pl.ds(pl.multiple_of(chip * 2 * rows, 128), 2 * rows)], lbuf, lsem)
        return a, o, b, lc

    copy(0, 0).start()
    own_out(0)
    for bt in range(nb):
        rz(bt).start()
    own_out(1)
    for k in range(1, nf):
        copy(0, k).start()

    def zero(i, carry):
        for c in range(12):
            t_ref[i, c] = jnp.zeros(t_ref.shape[2:], F32)
        return carry
    lax.fori_loop(0, nf, zero, 0)

    got(0, 0).wait_recv()
    _, o, b, lc = xload(0, 0, 0)
    o.start()
    b.start()
    lc.start()

    def unit(i, carry):
        slot = lax.rem(i, 2)
        rel, k = table(i, [u[0] for u in UNITS]), table(i, [u[1] for u in UNITS])
        nrel, nk = table(i, [u[0] for u in UNITS[1:]] + [0]), table(i, [u[1] for u in UNITS[1:]] + [0])
        for j, acts in events.items():
            if acts:
                @pl.when(i == j)
                def _():
                    for act in acts:
                        act()
        a, o, b, lc = xload(slot, rel, k)
        a.wait()
        b.wait()
        lc.wait()
        for c3 in range(3):
            for u in range(3):
                cs = slice(c3 * 256, (c3 + 1) * 256)
                hi, mid, low = split3(lbuf[u, :, cs])
                lsp[0, u, :, cs] = hi
                lsp[1, u, :, cs] = mid
                lsp[2, u, :, cs] = low

        @pl.when(i + 1 < len(UNITS))
        def _():
            for n, kind in ((OWN, (0,)), (XN, (5,)), (YN, (6,)), (DN, (7,))):
                @pl.when(nrel == n)
                def _():
                    for kd in kind:
                        got(kd, nk).wait_recv()
            na, no, nbb, nl = xload(1 - slot, nrel, nk)

            @pl.when(nrel == OWN)
            def _():
                no.start()

            @pl.when(nrel != OWN)
            def _():
                na.start()
            nbb.start()
            nl.start()
        for p in range(2):
            for q in range(2):
                xs = jnp.concatenate([xbuf[slot, 0, :, p, q, :], xbuf[slot, 1, :, p, q, :]], axis=0)
                xparts = split3(xs)
                for u in range(3):
                    idx = (u * 2 + p) * 2 + q
                    t_ref[k, idx] = dot6([lsp[j, u] for j in range(3)], xparts, 0) + t_ref[k, idx]

        @pl.when(rel == DN)
        def _():
            mix(k)
        return carry

    def mix(k):
        w = [w_ref[j] for j in range(36)]

        def wt(u, s, p, v):
            return w[((u * 2 + s) * 2 + p) * 3 + v]

        def rows8(j, carry):
            for h in range(FB // 128):
                sl = (pl.ds(pl.multiple_of(j * 8, 8), 8), slice(h * 128, (h + 1) * 128))
                t = [t_ref[(k, c) + sl] for c in range(12)]
                md = {}
                for s in range(2):
                    for v in range(3):
                        for q in range(2):
                            terms = [t[(u * 2 + p) * 2 + q] * wt(u, s, p, v) for u in range(3) for p in range(2)]
                            md[s, v, q] = functools.reduce(lambda m, n: m + n, terms)
                for s in range(2):
                    for tt in range(2):
                        for r in range(3):
                            terms = [md[s, v, q] * wt(v, tt, q, r) for v in range(3) for q in range(2)]
                            t_ref[(k, (s * 2 + tt) * 3 + r) + sl] = functools.reduce(lambda m, n: m + n, terms)
            return carry
        lax.fori_loop(0, rows // 8, rows8, 0)

    lax.fori_loop(0, len(UNITS), unit, 0)

    ntile = 2 * nb
    nunit = ntile * nf

    def rload(slot, j):
        tile = j // nf
        k = lax.rem(j, nf)
        bt = lax.rem(tile, nb)
        rws = pl.ds(pl.multiple_of(bt * BT, BT), BT)
        other = pltpu.make_async_copy(rx.at[:, rws, pl.ds(pl.multiple_of(k * FB, FB), FB)], rbuf.at[slot], bsem.at[slot])
        own = pltpu.make_async_copy(r_ref.at[:, rws, pl.ds(pl.multiple_of(z * cols + k * FB, FB), FB)], rbuf.at[slot],
                                    bsem.at[slot])
        return other, own

    rs(0, 1 - core).wait_recv()
    rload(0, 0)[0].start()
    event_r(2)

    def aflush(slot, bt):
        return pltpu.make_async_copy(acc.at[slot], ys.at[bt], asem)

    def yout(bt, h):
        return pltpu.make_async_copy(xbuf.at[0, h], y_ref.at[:, :, :, pl.ds(pl.multiple_of(bt * BT + h * FB, FB), FB)],
                                     osem.at[h])

    def yload(bt):
        return pltpu.make_async_copy(yr.at[bt], yrbuf, ysem)

    def unit2(j, carry):
        slot = lax.rem(j, 2)
        tile = j // nf
        k = lax.rem(j, nf)
        bt = lax.rem(tile, nb)
        aslot = lax.rem(tile, 2)

        @pl.when(k == 0)
        def _():
            for st in range(4):
                acc[aslot, st] = jnp.zeros(acc.shape[2:], F32)
        rload(slot, j)[0].wait()
        for bt_ in range(1, nb):
            @pl.when(j + 1 == bt_ * nf)
            def _():
                rs(bt_, 1 - core).wait_recv()

        @pl.when(j + 1 < nb * nf)
        def _():
            rload(1 - slot, j + 1)[0].start()

        @pl.when(jnp.logical_and(j + 1 >= nb * nf, j + 1 < nunit))
        def _():
            rload(1 - slot, j + 1)[1].start()

        @pl.when(jnp.logical_and(tile >= nb, k == nf - 1))
        def _():
            yz(bt).wait_recv()
            yload(bt).start()
        rparts = [split3(rbuf[slot, r]) for r in range(3)]
        for st in range(4):
            tot = acc[aslot, st]
            for r in range(3):
                tot = dot6(split3(t_ref[k, st * 3 + r]), rparts[r], 1) + tot
            acc[aslot, st] = tot

        @pl.when(jnp.logical_and(jnp.logical_and(tile >= 1, tile <= nb), k == 0))
        def _():
            aflush(1 - aslot, tile - 1).wait()
            yz(tile - 1).start()

        @pl.when(jnp.logical_and(tile < nb, k == nf - 1))
        def _():
            aflush(aslot, bt).start()

        @pl.when(jnp.logical_and(tile >= nb, k == nf - 1))
        def _():
            yload(bt).wait()

            @pl.when(tile > nb)
            def _():
                for h in range(2):
                    yout(bt - 1, h).wait()
            for s in range(2):
                for tt in range(2):
                    for h in range(2):
                        cs = slice(h * FB, (h + 1) * FB)
                        xbuf[0, h, :, s, tt, :] = acc[aslot, s * 2 + tt, :, cs] + yrbuf[s * 2 + tt, :, cs]
            for h in range(2):
                yout(bt, h).start()
        return carry

    lax.fori_loop(0, nunit, unit2, 0)
    for h in range(2):
        yout(nb - 1, h).wait()
    for bt in range(nb):
        rz(bt).wait_send()
        rs(bt, core).wait_send()
        yz(bt).wait_send()
    for k in range(nf):
        for kind in range(8):
            copy(kind, k).wait_send()


def apply_local(x, left, w, right):
    rows, cols = x.shape[0], x.shape[3]
    lt = jnp.transpose(left, (1, 0, 2))
    rt = jnp.transpose(right, (1, 0, 2))
    nf, nb = cols // FB, cols // BT
    hbm = pl.BlockSpec(memory_space=pltpu.HBM)
    S = jax.ShapeDtypeStruct
    dma = pltpu.SemaphoreType.DMA
    out = pl.pallas_call(
        kernel,
        out_shape=[S(x.shape, F32), S((8,) + x.shape, F32), S((3, cols, cols), F32), S((nb, 4, rows, BT), F32),
                   S((nb, 4, rows, BT), F32)],
        in_specs=[hbm, hbm, hbm, pl.BlockSpec(memory_space=pltpu.SMEM)],
        out_specs=[hbm] * 5,
        scratch_shapes=[
            pltpu.VMEM((nf, 12, rows, FB), F32),
            pltpu.VMEM((2, 2, rows, 2, 2, FB), F32),
            pltpu.VMEM((3, rows, 2 * rows), F32),
            pltpu.VMEM((3, 3, rows, 2 * rows), BF),
            pltpu.VMEM((2, 4, rows, BT), F32),
            pltpu.VMEM((2, 3, BT, FB), F32),
            pltpu.VMEM((4, rows, BT), F32),
            dma((8, nf)), dma((8, nf)), dma((nb,)), dma((nb,)), dma((nb,)), dma((nb,)), dma((nb,)), dma((nb,)),
            dma((2, 2)), dma, dma((2,)), dma, dma, dma((2,)),
        ],
        compiler_params=pltpu.CompilerParams(collective_id=0, has_side_effects=True, vmem_limit_bytes=67043328),
        name="heff",
    )(x, lt, rt, w.reshape(36))
    return out[0]


def solution(mesh):
    return jax.shard_map(apply_local, mesh=mesh,
                         in_specs=(P('bx', None, None, 'by'), P('bx', None, None), P(), P('by', None, None)),
                         out_specs=P('bx', None, None, 'by'), check_vma=False)
```

```python
import functools
import jax
import jax.numpy as jnp
from jax import lax
from jax.experimental import pallas as pl
from jax.experimental.pallas import tpu as pltpu
from jax.sharding import PartitionSpec as P

MESH = pl.DeviceIdType.MESH
BF, F32 = jnp.bfloat16, jnp.float32
FB = 256
BT = 512

OWN, XN, YN, DN = 0, 1, 2, 3


def S(rel, k):
    return ('s', rel, k)


def Q(own, bt, pair):
    return ('t', own, bt, pair)


UNITS = [S(OWN, 0), S(OWN, 1), S(OWN, 2), S(OWN, 3), S(OWN, 4), S(XN, 0), S(YN, 0), S(OWN, 5), S(XN, 1), S(DN, 0), S(YN, 1)]
UNITS += [S(XN, 2), S(YN, 2), S(DN, 1), Q(0, 0, 0), S(XN, 3), S(YN, 3), S(DN, 2), Q(0, 1, 0), S(XN, 4), S(YN, 4), S(DN, 3)]
UNITS += [Q(0, 0, 1), S(XN, 5), S(YN, 5), S(DN, 4), S(DN, 5), Q(0, 0, 2)]
UNITS += [Q(0, 1, 1), Q(0, 1, 2)] + [Q(0, 2, pair) for pair in range(3)]
UNITS += [Q(1, bt, pair) for bt in range(3) for pair in range(3)]
MIX_AFTER = {S(DN, k): k for k in range(6)}
LATE = {S(XN, 5), S(DN, 5)}
AT = {
    S(OWN, 3): ['xy0', 'own2'], S(YN, 0): ['xy1', 'own3'], S(OWN, 5): ['d0'], S(YN, 1): ['r0'],
    S(XN, 2): ['d1'], S(XN, 3): ['d2'], S(YN, 3): ['r1'], S(XN, 4): ['d3'], Q(0, 0, 1): ['xy5'], S(XN, 5): ['d4'],
    S(DN, 4): ['d5'], S(DN, 5): ['r2'],
}
MID = {
    S(DN, 0): ['xy2', 'own4'], S(DN, 1): ['xy3', 'own5'], S(DN, 2): ['xy4'],
}


def split3(v):
    hi = v.astype(BF)
    rest = v - hi.astype(F32)
    mid = rest.astype(BF)
    low = (rest - mid.astype(F32)).astype(BF)
    return hi, mid, low


def dot6(a, b, rhs_dim):
    def d(i, j):
        return lax.dot_general(a[i], b[j], (((1,), (rhs_dim,)), ((), ())), preferred_element_type=F32)
    return d(0, 0) + d(1, 0) + d(2, 0) + d(0, 1) + d(1, 1) + d(0, 2)


def table(i, values):
    out = values[0]
    for k, v in enumerate(values):
        if v != values[0]:
            out = jnp.where(i == k, v, out)
    return out


def kernel(x_ref, l_ref, r_ref, w_ref, y_ref, xg, rx, ys, yr, lc_ref,
           t_ref, xbuf, lsp, acc, rbuf,
           ssem, rsem, zsend, zrecv, bsend, brecv, ysend, yrecv, xsem, lsem, csem, psem, bsem, asem, ysem, osem):
    z = lax.axis_index('by')
    me = lax.axis_index('bx')
    core = lax.rem(me, 2)
    cx = lax.rem(me // 2, 2)
    cy = me // 4
    rows, cols = x_ref.shape[0], x_ref.shape[3]
    nf, nb = cols // FB, cols // BT
    half = rows // 2
    hw = cols // 2

    def index(dx, dy, dc):
        return (lax.rem(cy + dy, 2) * 2 + lax.rem(cx + dx, 2)) * 2 + lax.rem(core + dc, 2)

    sib, xn, yn, dn = index(0, 0, 1), index(1, 0, 0), index(0, 1, 0), index(1, 1, 0)
    dev_s, dev_x, dev_y, dev_z = (z, sib), (z, xn), (z, yn), (1 - z, me)

    barrier = pltpu.get_barrier_semaphore()
    for dev in (dev_s, dev_x, dev_y, dev_z):
        pl.semaphore_signal(barrier, inc=1, device_id=dev, device_id_type=MESH)
    pl.semaphore_wait(barrier, 4)

    def remote(src, dst, send, recv, dev):
        return pltpu.make_async_remote_copy(src_ref=src, dst_ref=dst, send_sem=send, recv_sem=recv, device_id=dev,
                                            device_id_type=MESH)

    def piece(ref, k):
        return ref.at[:, :, :, pl.ds(pl.multiple_of(k * FB, FB), FB)]

    def block(kind):
        if kind < 3:
            return xg.at[me]
        if kind == 3:
            return xg.at[yn, pl.ds(0, half)]
        if kind == 4:
            return xg.at[xn, pl.ds(half, half)]
        return xg.at[(xn, yn, dn)[kind - 5]]

    def send(kind, k):
        dst = piece(block(kind), k) if kind or k > 1 else xbuf.at[k, core]
        src = piece(x_ref, k) if kind < 3 else dst
        dev = (dev_s, dev_x, dev_y, dev_x, dev_y, dev_s, dev_s, dev_s)[kind]
        return remote(src, dst, ssem.at[kind, k], rsem.at[kind, k], dev)

    def arrived(kind, k):
        ref = (xg.at[sib], xg.at[xn], xg.at[yn], xg.at[dn, pl.ds(0, half)], xg.at[dn, pl.ds(half, half)],
               xg.at[index(1, 0, 1)], xg.at[index(0, 1, 1)], xg.at[index(1, 1, 1)])[kind]
        part = piece(ref, k) if kind or not isinstance(k, int) else xbuf.at[k, 1 - core]
        remote(part, part, ssem.at[kind, k], rsem.at[kind, k], dev_s).wait_recv()

    def rz(bt):
        rws = pl.ds(bt * BT, BT)
        src = r_ref.at[:, rws, pl.ds(pl.multiple_of((1 - z) * cols + core * hw, 128), hw)]
        dst = rx.at[:, rws, pl.ds(pl.multiple_of(core * hw, 128), hw)]
        return remote(src, dst, zsend.at[bt], zrecv.at[bt], dev_z)

    def rs(bt, c):
        part = rx.at[:, pl.ds(pl.multiple_of(bt * BT, BT), BT), pl.ds(pl.multiple_of(c * hw, 128), hw)]
        return remote(part, part, bsend.at[bt], brecv.at[bt], dev_s)

    def yz(bt):
        return remote(ys.at[bt], yr.at[bt], ysend.at[bt], yrecv.at[bt], dev_z)

    def run(name):
        k = int(name[-1])
        if name[:-1] == 'own':
            send(1, k).start()
            send(2, k).start()
        elif name[:-1] == 'xy':
            arrived(1, k)
            send(4, k).start()
            send(5, k).start()
            arrived(2, k)
            send(3, k).start()
            send(6, k).start()
        elif name[:-1] == 'd':
            arrived(3, k)
            arrived(4, k)
            send(7, k).start()
        elif name[:-1] == 'r':
            rz(k).wait_recv()
            rs(k, core).start()
        elif name[:-1] == 'f':
            flush(0, k).wait()
            yz(k).start()
        elif name[:-1] == 'y':
            yz(k).wait_recv()
            yload(yslot[k], k).start()

    n = len(UNITS)
    xslot, lslot, lmode, rslot = [0] * n, [0] * n, [0] * n, [0] * n
    cnt, prev, ls, seen, rcnt = 0, None, 1, set(), 0
    writes = {}
    for i, u in enumerate(UNITS):
        if u[0] == 's':
            xslot[i] = cnt % 2
            cnt += 1
            if u[1] != prev:
                ls = 1 - ls
                lmode[i] = 2 if u[1] in seen else 1
                if lmode[i] == 1:
                    nxt = next(j for j in range(i + 1, n) if UNITS[j][0] == 's')
                    writes[nxt] = u[1]
                seen.add(u[1])
                prev = u[1]
            lslot[i] = ls
        else:
            rslot[i] = rcnt % 2
            rcnt += 1
    lmode[0] = 0
    at = {i: list(AT.get(u, ())) for i, u in enumerate(UNITS)}
    mid = {i: list(MID.get(u, ())) for i, u in enumerate(UNITS)}
    mixk = [0 for u in UNITS]
    mixa = [MIX_AFTER.get(u, -1) + 1 for u in UNITS]
    init = [int(u[0] == 's' and all(v[0] != 's' or v[2] != u[2] for v in UNITS[:i])) for i, u in enumerate(UNITS)]
    sums = [i for i, u in enumerate(UNITS) if u[0] == 't']
    aslot, first, last = [0] * n, [0] * n, [0] * n
    order, yslot = [], {}
    for i in sums:
        tile = UNITS[i][1:3]
        if tile not in order:
            order.append(tile)
            first[i] = 1
        aslot[i] = order.index(tile) % 2
        yslot[tile[1]] = 1 - aslot[i]
        if all(UNITS[j][1:3] != tile for j in sums if j > i):
            last[i] = 1
            if tile[0] == 0:
                at[i + (1 if tile[1] == 0 else 2)].append('f%d' % tile[1])
            else:
                if tile[1] < nb - 1:
                    at[i].append('y%d' % tile[1])
    is_t = [int(u[0] == 't') for u in UNITS]
    arg = [[u[j] if len(u) > j else 0 for u in UNITS] for j in range(1, 4)]
    late = [int(u in LATE) for u in UNITS]

    def chip(rel):
        return lax.rem(cy + rel // 2, 2) * 2 + lax.rem(cx + lax.rem(rel, 2), 2)

    def xcopies(slot, rel, k):
        c = chip(rel) * 2
        return (pltpu.make_async_copy(piece(x_ref, k), xbuf.at[slot, core], xsem.at[slot, 0]),
                pltpu.make_async_copy(piece(xg.at[c + core], k), xbuf.at[slot, core], xsem.at[slot, 0]),
                pltpu.make_async_copy(piece(xg.at[c + 1 - core], k), xbuf.at[slot, 1 - core], xsem.at[slot, 1]))

    def xstart(slot, rel, k):
        own, far, sibling = xcopies(slot, rel, k)

        @pl.when(rel == OWN)
        def _():
            own.start()

        @pl.when(rel != OWN)
        def _():
            far.start()
        for r, kind in ((OWN, 0), (XN, 5), (YN, 6), (DN, 7)):
            @pl.when(rel == r)
            def _():
                arrived(kind, k)
        sibling.start()

    def lcopies(rel, what):
        base = chip(rel) * 2 * rows
        for j, (dst, off, width) in enumerate(((acc.at[0, pl.ds(0, 3)], 0, BT), (acc.at[1, pl.ds(0, 3), :, pl.ds(0, FB)], BT, FB))):
            src = l_ref.at[:, :, pl.ds(pl.multiple_of(base + off, 128), width)]
            getattr(pltpu.make_async_copy(src, dst, lsem.at[j]), what)()

    def cload(slot, rel):
        return pltpu.make_async_copy(lc_ref.at[rel], lsp.at[slot], csem)

    def cstore(slot, rel):
        return pltpu.make_async_copy(lsp.at[slot], lc_ref.at[rel], psem)

    def rcopies(slot, bt, pair):
        rws = pl.ds(pl.multiple_of(bt * BT, BT), BT)
        return (pltpu.make_async_copy(rx.at[:, rws, pl.ds(pl.multiple_of(pair * 512, 512), 512)], rbuf.at[slot], bsem.at[slot]),
                pltpu.make_async_copy(r_ref.at[:, rws, pl.ds(pl.multiple_of(z * cols + pair * 512, 512), 512)], rbuf.at[slot],
                                      bsem.at[slot]))

    def flush(slot, bt):
        return pltpu.make_async_copy(acc.at[slot], ys.at[bt], asem)

    def yload(slot, bt):
        return pltpu.make_async_copy(yr.at[bt], acc.at[slot], ysem)

    def yout(bt, h):
        return pltpu.make_async_copy(xbuf.at[1, h], y_ref.at[:, :, :, pl.ds(pl.multiple_of(bt * BT + h * FB, FB), FB)],
                                     osem.at[h])

    def lsplit(slot):
        def body(j, carry):
            sl = pl.ds(pl.multiple_of(j * 16, 16), 16)
            for u in range(3):
                for j, (off, width) in enumerate(((0, BT), (BT, FB))):
                    for part, v in enumerate(split3(acc[j, u, sl, :width])):
                        lsp[slot, part, u, sl, off:off + width] = v
            return carry
        lax.fori_loop(0, rows // 16, body, 0, unroll=2)

    for k in range(2):
        send(0, k).start()
    lcopies(OWN, 'start')
    for k in range(2):
        xcopies(k, OWN, k)[0].start()
    run('own0')
    for bt in range(nb):
        rz(bt).start()
    run('own1')
    for k in range(2, nf):
        send(0, k).start()
    lcopies(OWN, 'wait')
    lsplit(0)
    cstore(0, OWN).start()
    xcopies(0, OWN, 0)[0].wait()
    arrived(0, 0)

    def mix8(k, row):
        w = {(u, s, p, v): w_ref[u, s, p, v] for u in range(3) for s in range(2) for p in range(2) for v in range(3)}

        def wt(u, s, p, v):
            return w[u, s, p, v]

        for h in range(FB // 128):
            sl = (pl.ds(pl.multiple_of(row, 8), 8), slice(h * 128, (h + 1) * 128))
            t = [t_ref[(k, c) + sl] for c in range(12)]
            md = {}
            for s in range(2):
                for v in range(3):
                    for q in range(2):
                        terms = [t[(u * 2 + p) * 2 + q] * wt(u, s, p, v) for u in range(3) for p in range(2)]
                        md[s, v, q] = functools.reduce(lambda m, o: m + o, terms)
            for s in range(2):
                for tt in range(2):
                    for r in range(3):
                        terms = [md[s, v, q] * wt(v, tt, q, r) for v in range(3) for q in range(2)]
                        t_ref[(k, (s * 2 + tt) * 3 + r) + sl] = functools.reduce(lambda m, o: m + o, terms)

    writes = set(writes)
    fields = [(is_t, 2), (arg[0], 4), (arg[1], 8), (arg[2], 4), (xslot, 2), (lslot, 2), (lmode, 4), (rslot, 2), (aslot, 2),
              (first, 2), (last, 2), (late, 2), ([int(bool(at[i]) or i in writes) for i in range(n)], 2),
              ([int(bool(mid[i])) for i in range(n)], 2), (mixk, 8), (mixa, 8), (init, 2)]
    codes = []
    for i in range(n):
        code = 0
        for values, base in reversed(fields):
            code = code * base + values[i]
        codes.append(code)

    def decode(code):
        out = []
        for _, base in fields:
            out.append(jnp.bitwise_and(code, base - 1))
            code = jnp.right_shift(code, base.bit_length() - 1)
        return out

    def unit(i, code):
        kind, a0, a1, a2, xs_, ls_, lm_, rs_, as_, first_, last_, late_, ev_, evm_, mixk_, mixa_, init_ = decode(code)
        code1 = table(i, codes[1:] + [0])
        kind1, b0, b1, b2, xs1, ls1, lm1, rs1, _, first1, _, late1 = decode(code1)[:12]

        @pl.when(ev_ == 1)
        def _():
            for j in range(n):
                if at[j] or j in writes:
                    @pl.when(i == j)
                    def _():
                        if j in writes:
                            cstore(0, 0).wait()
                        for name in at[j]:
                            run(name)

        @pl.when(kind == 0)
        def _():
            @pl.when(late_ == 1)
            def _():
                xstart(xs_, a0, a1)
            @pl.when(i == 1)
            def _():
                xcopies(1, OWN, 1)[0].wait()
                arrived(0, 1)

            @pl.when(i > 1)
            def _():
                _, far, sibling = xcopies(xs_, a0, a1)
                far.wait()
                sibling.wait()

            @pl.when(lm_ == 1)
            def _():
                lcopies(a0, 'wait')
                lsplit(ls_)
                cstore(ls_, a0).start()

            @pl.when(lm_ == 2)
            def _():
                cload(ls_, a0).wait()

        @pl.when(kind == 1)
        def _():
            rcopies(rs_, a1, a2)[0].wait()

        def ahead():
            @pl.when(kind1 == 0)
            def _():
                @pl.when(jnp.logical_and(late1 == 0, i > 0))
                def _():
                    xstart(xs1, b0, b1)

                @pl.when(lm1 == 1)
                def _():
                    lcopies(b0, 'start')

                @pl.when(lm1 == 2)
                def _():
                    cload(ls1, b0).start()

            @pl.when(kind1 == 1)
            def _():
                @pl.when(b0 == 0)
                def _():
                    @pl.when(first1 == 1)
                    def _():
                        rs(b1, 1 - core).wait_recv()
                    rcopies(rs1, b1, b2)[0].start()

                @pl.when(b0 == 1)
                def _():
                    rcopies(rs1, b1, b2)[1].start()

        @pl.when(i + 1 < n)
        def _():
            ahead()

        @pl.when(kind == 0)
        def _():
            for p in range(2):
                for q in range(2):
                    xs = jnp.concatenate([xbuf[xs_, 0, :, p, q, :], xbuf[xs_, 1, :, p, q, :]], axis=0)
                    xparts = split3(xs)
                    for u in range(3):
                        idx = (u * 2 + p) * 2 + q
                        old = jnp.where(init_ == 1, 0.0, t_ref[a1, idx])
                        t_ref[a1, idx] = dot6([lsp[ls_, j, u] for j in range(3)], xparts, 0) + old

        @pl.when(evm_ == 1)
        def _():
            for j in range(n):
                if mid[j]:
                    @pl.when(i == j)
                    def _():
                        for name in mid[j]:
                            run(name)

        @pl.when(mixa_ > 0)
        def _():
            def body(j, carry):
                mix8(mixa_ - 1, j * 8)
                return carry
            lax.fori_loop(0, rows // 8, body, 0, unroll=4)

        @pl.when(kind == 1)
        def _():
            rparts = [[split3(rbuf[rs_, r, :, f * FB:(f + 1) * FB]) for f in range(2)] for r in range(3)]
            for st in range(4):
                tot = jnp.where(first_ == 1, 0.0, acc[as_, st])
                for r in range(3):
                    for f in range(2):
                        tot = dot6(split3(t_ref[a2 * 2 + f, st * 3 + r]), rparts[r][f], 1) + tot
                acc[as_, st] = tot

            @pl.when(last_ == 1)
            def _():
                @pl.when(a0 == 0)
                def _():
                    flush(as_, a1).start()

                @pl.when(a0 == 1)
                def _():
                    @pl.when(i == n - 1)
                    def _():
                        run('y%d' % (nb - 1))

                    @pl.when(a1 > 0)
                    def _():
                        for h in range(2):
                            yout(a1 - 1, h).wait()
                    yload(1 - as_, a1).wait()
                    for h in range(2):
                        for s in range(2):
                            for tt in range(2):
                                st = s * 2 + tt
                                part = acc[1 - as_, st, :, h * FB:(h + 1) * FB]
                                xbuf[1, h, :, s, tt, :] = acc[as_, st, :, h * FB:(h + 1) * FB] + part
                        yout(a1, h).start()
        return code1

    lax.fori_loop(0, n, unit, jnp.int32(codes[0]))
    for h in range(2):
        yout(nb - 1, h).wait()
    for bt in range(nb):
        rz(bt).wait_send()
        rs(bt, core).wait_send()
        yz(bt).wait_send()
    for k in range(nf):
        for kd in range(8):
            send(kd, k).wait_send()


def apply_local(x, left, w, right):
    rows, cols = x.shape[0], x.shape[3]
    lt = jnp.transpose(left, (1, 0, 2))
    rt = jnp.transpose(right, (1, 0, 2))
    nf, nb = cols // FB, cols // BT
    hbm = pl.BlockSpec(memory_space=pltpu.HBM)
    shape = jax.ShapeDtypeStruct
    dma = pltpu.SemaphoreType.DMA
    tiles = shape((nb, 4, rows, BT), F32)
    out = pl.pallas_call(
        kernel,
        out_shape=[shape(x.shape, F32), shape((8,) + x.shape, F32), shape((3, cols, cols), F32), tiles, tiles,
                   shape((4, 3, 3, rows, 2 * rows), BF)],
        in_specs=[hbm, hbm, hbm, pl.BlockSpec(memory_space=pltpu.SMEM)],
        out_specs=[hbm] * 6,
        scratch_shapes=[
            pltpu.VMEM((nf, 12, rows, FB), F32),
            pltpu.VMEM((2, 2, rows, 2, 2, FB), F32),
            pltpu.VMEM((2, 3, 3, rows, 2 * rows), BF),
            pltpu.VMEM((2, 4, rows, BT), F32),
            pltpu.VMEM((2, 3, BT, 512), F32),
            dma((8, nf)), dma((8, nf)), dma((nb,)), dma((nb,)), dma((nb,)), dma((nb,)), dma((nb,)), dma((nb,)),
            dma((2, 2)), dma((2,)), dma, dma, dma((2,)), dma, dma, dma((2,)),
        ],
        compiler_params=pltpu.CompilerParams(collective_id=0, has_side_effects=True, vmem_limit_bytes=67043328),
        name="heff",
    )(x, lt, rt, w)
    return out[0]


def solution(mesh):
    return jax.shard_map(apply_local, mesh=mesh,
                         in_specs=(P('bx', None, None, 'by'), P('bx', None, None), P(), P('by', None, None)),
                         out_specs=P('bx', None, None, 'by'), check_vma=False)
```

```python
import functools
import jax
import jax.numpy as jnp
from jax import lax
from jax.experimental import pallas as pl
from jax.experimental.pallas import tpu as pltpu
from jax.sharding import PartitionSpec as P

MESH = pl.DeviceIdType.MESH
BF, F32 = jnp.bfloat16, jnp.float32
FB = 256
BT = 512

OWN, XN, YN, DN = 0, 1, 2, 3


def S(rel, k):
    return ('s', rel, k)


def Q(own, bt, pair):
    return ('t', own, bt, pair)


UNITS = [S(OWN, 0), S(OWN, 1), S(OWN, 2), S(OWN, 3), S(OWN, 4), S(XN, 0), S(YN, 0), S(OWN, 5), S(XN, 1), S(DN, 0), S(YN, 1)]
UNITS += [S(XN, 2), S(YN, 2), S(DN, 1), Q(0, 0, 0), S(XN, 3), S(YN, 3), S(DN, 2), Q(0, 1, 0), S(XN, 4), S(YN, 4), S(DN, 3)]
UNITS += [Q(0, 0, 1), S(XN, 5), S(YN, 5), S(DN, 4), S(DN, 5), Q(0, 0, 2)]
UNITS += [Q(0, 1, 1), Q(0, 1, 2)] + [Q(0, 2, pair) for pair in range(3)]
UNITS += [Q(1, bt, pair) for bt in range(3) for pair in range(3)]
MIX_AFTER = {S(DN, k): k for k in range(6)}
LATE = {S(DN, 5)}
AT = {
    S(OWN, 3): ['xy0', 'own2'], S(YN, 0): ['xy1', 'own3'], S(OWN, 5): ['d0'], S(YN, 1): ['r0'],
    S(XN, 2): ['d1'], S(XN, 3): ['d2'], S(YN, 3): ['r1'], S(XN, 4): ['d3'], S(XN, 5): ['d4'],
    S(DN, 4): ['d5'], S(DN, 5): ['r2'],
}
MID = {
    S(DN, 0): ['xy2', 'own4'], S(DN, 1): ['xy3', 'own5'], S(DN, 2): ['xy4'], S(DN, 3): ['xy5'],
    S(DN, 4): ['load5'],
}


def split3(v):
    hi = v.astype(BF)
    rest = v - hi.astype(F32)
    mid = rest.astype(BF)
    low = (rest - mid.astype(F32)).astype(BF)
    return hi, mid, low


def dot6(a, b, rhs_dim):
    def d(i, j):
        return lax.dot_general(a[i], b[j], (((1,), (rhs_dim,)), ((), ())), preferred_element_type=F32)
    return d(0, 0) + d(1, 0) + d(2, 0) + d(0, 1) + d(1, 1) + d(0, 2)


def table(i, values):
    out = values[0]
    for k, v in enumerate(values):
        if v != values[0]:
            out = jnp.where(i == k, v, out)
    return out


def kernel(x_ref, l_ref, r_ref, w_ref, y_ref, xg, rx, ys, yr, lc_ref,
           t_ref, xbuf, lsp, acc, rbuf,
           ssem, rsem, zsend, zrecv, bsend, brecv, ysend, yrecv, xsem, lsem, csem, psem, bsem, asem, ysem, osem):
    z = lax.axis_index('by')
    me = lax.axis_index('bx')
    core = lax.rem(me, 2)
    cx = lax.rem(me // 2, 2)
    cy = me // 4
    rows, cols = x_ref.shape[0], x_ref.shape[3]
    nf, nb = cols // FB, cols // BT
    half = rows // 2
    hw = cols // 2

    def index(dx, dy, dc):
        return (lax.rem(cy + dy, 2) * 2 + lax.rem(cx + dx, 2)) * 2 + lax.rem(core + dc, 2)

    sib, xn, yn, dn = index(0, 0, 1), index(1, 0, 0), index(0, 1, 0), index(1, 1, 0)
    dev_s, dev_x, dev_y, dev_z = (z, sib), (z, xn), (z, yn), (1 - z, me)

    def remote(src, dst, send, recv, dev):
        return pltpu.make_async_remote_copy(src_ref=src, dst_ref=dst, send_sem=send, recv_sem=recv, device_id=dev,
                                            device_id_type=MESH)

    def piece(ref, k):
        return ref.at[:, :, :, pl.ds(pl.multiple_of(k * FB, FB), FB)]

    def block(kind):
        if kind < 3:
            return xg.at[me]
        if kind == 3:
            return xg.at[yn, pl.ds(0, half)]
        if kind == 4:
            return xg.at[xn, pl.ds(half, half)]
        return xg.at[(xn, yn, dn)[kind - 5]]

    def send(kind, k):
        dst = piece(block(kind), k) if kind or k > 1 else xbuf.at[k, core]
        src = piece(x_ref, k) if kind < 3 else dst
        dev = (dev_s, dev_x, dev_y, dev_x, dev_y, dev_s, dev_s, dev_s)[kind]
        return remote(src, dst, ssem.at[kind, k], rsem.at[kind, k], dev)

    def arrived(kind, k):
        ref = (xg.at[sib], xg.at[xn], xg.at[yn], xg.at[dn, pl.ds(0, half)], xg.at[dn, pl.ds(half, half)],
               xg.at[index(1, 0, 1)], xg.at[index(0, 1, 1)], xg.at[index(1, 1, 1)])[kind]
        part = piece(ref, k) if kind or not isinstance(k, int) else xbuf.at[k, 1 - core]
        remote(part, part, ssem.at[kind, k], rsem.at[kind, k], dev_s).wait_recv()

    def rz(bt):
        rws = pl.ds(bt * BT, BT)
        src = r_ref.at[:, rws, pl.ds(pl.multiple_of((1 - z) * cols + core * hw, 128), hw)]
        dst = rx.at[:, rws, pl.ds(pl.multiple_of(core * hw, 128), hw)]
        return remote(src, dst, zsend.at[bt], zrecv.at[bt], dev_z)

    def rs(bt, c):
        part = rx.at[:, pl.ds(pl.multiple_of(bt * BT, BT), BT), pl.ds(pl.multiple_of(c * hw, 128), hw)]
        return remote(part, part, bsend.at[bt], brecv.at[bt], dev_s)

    def yz(bt):
        return remote(ys.at[bt], yr.at[bt], ysend.at[bt], yrecv.at[bt], dev_z)

    def run(name):
        k = int(name[-1])
        if name[:-1] == 'own':
            send(1, k).start()
            send(2, k).start()
        elif name[:-1] == 'xy':
            arrived(1, k)
            send(4, k).start()
            send(5, k).start()
            arrived(2, k)
            send(3, k).start()
            send(6, k).start()
        elif name[:-1] == 'd':
            arrived(3, k)
            arrived(4, k)
            send(7, k).start()
        elif name[:-1] == 'r':
            rz(k).wait_recv()
            rs(k, core).start()
        elif name[:-1] == 'load':
            xstart(xslot[UNITS.index(S(DN, k))], DN, k)
        elif name[:-1] == 'f':
            flush(0, k).wait()
            yz(k).start()
        elif name[:-1] == 'y':
            yz(k).wait_recv()
            yload(yslot[k], k).start()

    n = len(UNITS)
    xslot, lslot, lmode, rslot = [0] * n, [0] * n, [0] * n, [0] * n
    cnt, prev, ls, seen, rcnt = 0, None, 1, set(), 0
    writes = {}
    for i, u in enumerate(UNITS):
        if u[0] == 's':
            xslot[i] = cnt % 2
            cnt += 1
            if u[1] != prev:
                ls = 1 - ls
                lmode[i] = 2 if u[1] in seen else 1
                if lmode[i] == 1:
                    nxt = next(j for j in range(i + 1, n) if UNITS[j][0] == 's')
                    writes[nxt] = u[1]
                seen.add(u[1])
                prev = u[1]
            lslot[i] = ls
        else:
            rslot[i] = rcnt % 2
            rcnt += 1
    lmode[0] = 0
    at = {i: list(AT.get(u, ())) for i, u in enumerate(UNITS)}
    mid = {i: list(MID.get(u, ())) for i, u in enumerate(UNITS)}
    mixk = [0 for u in UNITS]
    mixa = [MIX_AFTER.get(u, -1) + 1 for u in UNITS]
    init = [int(u[0] == 's' and all(v[0] != 's' or v[2] != u[2] for v in UNITS[:i])) for i, u in enumerate(UNITS)]
    sums = [i for i, u in enumerate(UNITS) if u[0] == 't']
    aslot, first, last = [0] * n, [0] * n, [0] * n
    order, yslot = [], {}
    for i in sums:
        tile = UNITS[i][1:3]
        if tile not in order:
            order.append(tile)
            first[i] = 1
        aslot[i] = order.index(tile) % 2
        yslot[tile[1]] = 1 - aslot[i]
        if all(UNITS[j][1:3] != tile for j in sums if j > i):
            last[i] = 1
            if tile[0] == 0:
                at[i + (1 if tile[1] == 0 else 2)].append('f%d' % tile[1])
            else:
                if tile[1] < nb - 1:
                    at[i].append('y%d' % tile[1])
    is_t = [int(u[0] == 't') for u in UNITS]
    arg = [[u[j] if len(u) > j else 0 for u in UNITS] for j in range(1, 4)]
    late = [int(u in LATE) for u in UNITS]

    def chip(rel):
        return lax.rem(cy + rel // 2, 2) * 2 + lax.rem(cx + lax.rem(rel, 2), 2)

    def xcopies(slot, rel, k):
        c = chip(rel) * 2
        return (pltpu.make_async_copy(piece(x_ref, k), xbuf.at[slot, core], xsem.at[slot, 0]),
                pltpu.make_async_copy(piece(xg.at[c + core], k), xbuf.at[slot, core], xsem.at[slot, 0]),
                pltpu.make_async_copy(piece(xg.at[c + 1 - core], k), xbuf.at[slot, 1 - core], xsem.at[slot, 1]))

    def xstart(slot, rel, k):
        rel = jnp.int32(rel)
        own, far, sibling = xcopies(slot, rel, k)

        @pl.when(rel == OWN)
        def _():
            own.start()

        @pl.when(rel != OWN)
        def _():
            far.start()
        for r, kind in ((OWN, 0), (XN, 5), (YN, 6), (DN, 7)):
            @pl.when(rel == r)
            def _():
                arrived(kind, k)
        sibling.start()

    def lcopies(rel, what):
        base = chip(rel) * 2 * rows
        for j, (dst, off, width) in enumerate(((acc.at[0, pl.ds(0, 3)], 0, BT), (acc.at[1, pl.ds(0, 3), :, pl.ds(0, FB)], BT, FB))):
            src = l_ref.at[:, :, pl.ds(pl.multiple_of(base + off, 128), width)]
            getattr(pltpu.make_async_copy(src, dst, lsem.at[j]), what)()

    def cload(slot, rel):
        return pltpu.make_async_copy(lc_ref.at[rel], lsp.at[slot], csem)

    def cstore(slot, rel):
        return pltpu.make_async_copy(lsp.at[slot], lc_ref.at[rel], psem)

    def rcopies(slot, bt, pair):
        rws = pl.ds(pl.multiple_of(bt * BT, BT), BT)
        return (pltpu.make_async_copy(rx.at[:, rws, pl.ds(pl.multiple_of(pair * 512, 512), 512)], rbuf.at[slot], bsem.at[slot]),
                pltpu.make_async_copy(r_ref.at[:, rws, pl.ds(pl.multiple_of(z * cols + pair * 512, 512), 512)], rbuf.at[slot],
                                      bsem.at[slot]))

    def flush(slot, bt):
        return pltpu.make_async_copy(acc.at[slot], ys.at[bt], asem)

    def yload(slot, bt):
        return pltpu.make_async_copy(yr.at[bt], acc.at[slot], ysem)

    def yout(bt, h):
        return pltpu.make_async_copy(xbuf.at[1, h], y_ref.at[:, :, :, pl.ds(pl.multiple_of(bt * BT + h * FB, FB), FB)],
                                     osem.at[h])

    def lsplit(slot):
        def body(j, carry):
            sl = pl.ds(pl.multiple_of(j * 16, 16), 16)
            for u in range(3):
                for j, (off, width) in enumerate(((0, BT), (BT, FB))):
                    for part, v in enumerate(split3(acc[j, u, sl, :width])):
                        lsp[slot, part, u, sl, off:off + width] = v
            return carry
        lax.fori_loop(0, rows // 16, body, 0, unroll=2)

    lcopies(OWN, 'start')
    for k in range(2):
        xcopies(k, OWN, k)[0].start()
    barrier = pltpu.get_barrier_semaphore()
    for dev in (dev_s, dev_x, dev_y, dev_z):
        pl.semaphore_signal(barrier, inc=1, device_id=dev, device_id_type=MESH)
    pl.semaphore_wait(barrier, 4)
    for k in range(2):
        send(0, k).start()
    run('own0')
    for bt in range(nb):
        rz(bt).start()
    run('own1')
    for k in range(2, nf):
        send(0, k).start()
    lcopies(OWN, 'wait')
    lsplit(0)
    cstore(0, OWN).start()
    xcopies(0, OWN, 0)[0].wait()
    arrived(0, 0)

    def mix8(k, row):
        w = {(u, s, p, v): w_ref[u, s, p, v] for u in range(3) for s in range(2) for p in range(2) for v in range(3)}

        def wt(u, s, p, v):
            return w[u, s, p, v]

        for h in range(FB // 128):
            sl = (pl.ds(pl.multiple_of(row, 8), 8), slice(h * 128, (h + 1) * 128))
            t = [t_ref[(k, c) + sl] for c in range(12)]
            md = {}
            for s in range(2):
                for v in range(3):
                    for q in range(2):
                        terms = [t[(u * 2 + p) * 2 + q] * wt(u, s, p, v) for u in range(3) for p in range(2)]
                        md[s, v, q] = functools.reduce(lambda m, o: m + o, terms)
            for s in range(2):
                for tt in range(2):
                    for r in range(3):
                        terms = [md[s, v, q] * wt(v, tt, q, r) for v in range(3) for q in range(2)]
                        t_ref[(k, (s * 2 + tt) * 3 + r) + sl] = functools.reduce(lambda m, o: m + o, terms)

    writes = set(writes)
    fields = [(is_t, 2), (arg[0], 4), (arg[1], 8), (arg[2], 4), (xslot, 2), (lslot, 2), (lmode, 4), (rslot, 2), (aslot, 2),
              (first, 2), (last, 2), (late, 2), ([int(bool(at[i]) or i in writes) for i in range(n)], 2),
              ([int(bool(mid[i])) for i in range(n)], 2), (mixk, 8), (mixa, 8), (init, 2)]
    codes = []
    for i in range(n):
        code = 0
        for values, base in reversed(fields):
            code = code * base + values[i]
        codes.append(code)

    def decode(code):
        out = []
        for _, base in fields:
            out.append(jnp.bitwise_and(code, base - 1))
            code = jnp.right_shift(code, base.bit_length() - 1)
        return out

    def unit(i, code):
        kind, a0, a1, a2, xs_, ls_, lm_, rs_, as_, first_, last_, late_, ev_, evm_, mixk_, mixa_, init_ = decode(code)
        code1 = table(i, codes[1:] + [0])
        kind1, b0, b1, b2, xs1, ls1, lm1, rs1, _, first1, _, late1 = decode(code1)[:12]

        @pl.when(ev_ == 1)
        def _():
            for j in range(n):
                if at[j] or j in writes:
                    @pl.when(i == j)
                    def _():
                        if j in writes:
                            cstore(0, 0).wait()
                        for name in at[j]:
                            run(name)

        @pl.when(kind == 0)
        def _():
            @pl.when(i == 1)
            def _():
                xcopies(1, OWN, 1)[0].wait()
                arrived(0, 1)

            @pl.when(i > 1)
            def _():
                _, far, sibling = xcopies(xs_, a0, a1)
                far.wait()
                sibling.wait()

            @pl.when(lm_ == 1)
            def _():
                lcopies(a0, 'wait')
                lsplit(ls_)
                cstore(ls_, a0).start()

            @pl.when(lm_ == 2)
            def _():
                cload(ls_, a0).wait()

        @pl.when(kind == 1)
        def _():
            rcopies(rs_, a1, a2)[0].wait()

        def ahead():
            @pl.when(kind1 == 0)
            def _():
                @pl.when(jnp.logical_and(late1 == 0, i > 0))
                def _():
                    xstart(xs1, b0, b1)

                @pl.when(lm1 == 1)
                def _():
                    lcopies(b0, 'start')

                @pl.when(lm1 == 2)
                def _():
                    cload(ls1, b0).start()

            @pl.when(kind1 == 1)
            def _():
                @pl.when(b0 == 0)
                def _():
                    @pl.when(first1 == 1)
                    def _():
                        rs(b1, 1 - core).wait_recv()
                    rcopies(rs1, b1, b2)[0].start()

                @pl.when(b0 == 1)
                def _():
                    rcopies(rs1, b1, b2)[1].start()

        @pl.when(i + 1 < n)
        def _():
            ahead()

        @pl.when(kind == 0)
        def _():
            for p in range(2):
                for q in range(2):
                    xs = jnp.concatenate([xbuf[xs_, 0, :, p, q, :], xbuf[xs_, 1, :, p, q, :]], axis=0)
                    xparts = split3(xs)
                    for u in range(3):
                        idx = (u * 2 + p) * 2 + q
                        old = jnp.where(init_ == 1, 0.0, t_ref[a1, idx])
                        t_ref[a1, idx] = dot6([lsp[ls_, j, u] for j in range(3)], xparts, 0) + old

        @pl.when(evm_ == 1)
        def _():
            for j in range(n):
                if mid[j]:
                    @pl.when(i == j)
                    def _():
                        for name in mid[j]:
                            run(name)

        @pl.when(mixa_ > 0)
        def _():
            def body(j, carry):
                mix8(mixa_ - 1, j * 8)
                return carry
            lax.fori_loop(0, rows // 8, body, 0, unroll=4)

        @pl.when(kind == 1)
        def _():
            rparts = [[split3(rbuf[rs_, r, :, f * FB:(f + 1) * FB]) for f in range(2)] for r in range(3)]
            for st in range(4):
                tot = jnp.where(first_ == 1, 0.0, acc[as_, st])
                for r in range(3):
                    for f in range(2):
                        tot = dot6(split3(t_ref[a2 * 2 + f, st * 3 + r]), rparts[r][f], 1) + tot
                acc[as_, st] = tot

            @pl.when(last_ == 1)
            def _():
                @pl.when(a0 == 0)
                def _():
                    flush(as_, a1).start()

                @pl.when(a0 == 1)
                def _():
                    @pl.when(i == n - 1)
                    def _():
                        run('y%d' % (nb - 1))

                    @pl.when(a1 > 0)
                    def _():
                        for h in range(2):
                            yout(a1 - 1, h).wait()
                    yload(1 - as_, a1).wait()
                    for h in range(2):
                        for s in range(2):
                            for tt in range(2):
                                st = s * 2 + tt
                                part = acc[1 - as_, st, :, h * FB:(h + 1) * FB]
                                xbuf[1, h, :, s, tt, :] = acc[as_, st, :, h * FB:(h + 1) * FB] + part
                        yout(a1, h).start()
        return code1

    lax.fori_loop(0, n, unit, jnp.int32(codes[0]))
    for h in range(2):
        yout(nb - 1, h).wait()
    for bt in range(nb):
        rz(bt).wait_send()
        rs(bt, core).wait_send()
        yz(bt).wait_send()
    for k in range(nf):
        for kd in range(8):
            send(kd, k).wait_send()


def apply_local(x, left, w, right):
    rows, cols = x.shape[0], x.shape[3]
    lt = jnp.transpose(left, (1, 0, 2))
    rt = jnp.transpose(right, (1, 0, 2))
    nf, nb = cols // FB, cols // BT
    hbm = pl.BlockSpec(memory_space=pltpu.HBM)
    shape = jax.ShapeDtypeStruct
    dma = pltpu.SemaphoreType.DMA
    tiles = shape((nb, 4, rows, BT), F32)
    out = pl.pallas_call(
        kernel,
        out_shape=[shape(x.shape, F32), shape((8,) + x.shape, F32), shape((3, cols, cols), F32), tiles, tiles,
                   shape((4, 3, 3, rows, 2 * rows), BF)],
        in_specs=[hbm, hbm, hbm, pl.BlockSpec(memory_space=pltpu.SMEM)],
        out_specs=[hbm] * 6,
        scratch_shapes=[
            pltpu.VMEM((nf, 12, rows, FB), F32),
            pltpu.VMEM((2, 2, rows, 2, 2, FB), F32),
            pltpu.VMEM((2, 3, 3, rows, 2 * rows), BF),
            pltpu.VMEM((2, 4, rows, BT), F32),
            pltpu.VMEM((2, 3, BT, 512), F32),
            dma((8, nf)), dma((8, nf)), dma((nb,)), dma((nb,)), dma((nb,)), dma((nb,)), dma((nb,)), dma((nb,)),
            dma((2, 2)), dma((2,)), dma, dma, dma((2,)), dma, dma, dma((2,)),
        ],
        compiler_params=pltpu.CompilerParams(collective_id=0, has_side_effects=True, vmem_limit_bytes=67043328),
        name="heff",
    )(x, lt, rt, w)
    return out[0]


def solution(mesh):
    return jax.shard_map(apply_local, mesh=mesh,
                         in_specs=(P('bx', None, None, 'by'), P('bx', None, None), P(), P('by', None, None)),
                         out_specs=P('bx', None, None, 'by'), check_vma=False)
```

```python
import functools
import jax
import jax.numpy as jnp
from jax import lax
from jax.experimental import pallas as pl
from jax.experimental.pallas import tpu as pltpu
from jax.sharding import PartitionSpec as P

MESH = pl.DeviceIdType.MESH
BF, F32 = jnp.bfloat16, jnp.float32
FB = 256
BT = 512

OWN, XN, YN, DN = 0, 1, 2, 3


def S(rel, k):
    return ('s', rel, k)


def Q(own, bt, pair):
    return ('t', own, bt, pair)


UNITS = [S(OWN, 0), S(OWN, 1), S(OWN, 2), S(OWN, 3), S(OWN, 4), S(XN, 0), S(YN, 0), S(OWN, 5), S(XN, 1), S(YN, 1), S(DN, 0)]
UNITS += [S(XN, 2), S(YN, 2), S(DN, 1), Q(0, 0, 0), S(XN, 3), S(YN, 3), S(DN, 2), S(XN, 4), Q(0, 1, 0), S(YN, 4), S(DN, 3)]
UNITS += [Q(0, 0, 1), S(XN, 5), S(YN, 5), S(DN, 4), S(DN, 5), Q(0, 0, 2)]
UNITS += [Q(0, 1, 1), Q(0, 1, 2)] + [Q(0, 2, pair) for pair in range(3)]
UNITS += [Q(1, bt, pair) for bt in range(3) for pair in range(3)]
HALFWAY = {S(DN, 0), S(DN, 2)}
MIX_AFTER = {S(DN, k): k for k in range(6)}
LATE = {S(DN, 5), S(XN, 2), S(XN, 4)}
AT = {
    S(OWN, 3): ['xy0', 'own2'], S(YN, 0): ['xy1', 'own3'], S(XN, 1): ['d0'], S(DN, 0): ['r0'],
    S(XN, 2): ['d1'], S(XN, 3): ['d2'], S(DN, 2): ['r1'], Q(0, 1, 0): ['d3'], S(XN, 5): ['d4'],
    S(DN, 4): ['d5'], S(DN, 5): ['r2'],
}
MID = {
    S(DN, 0): ['xy2', 'own4'], S(DN, 1): ['xy3', 'own5'], S(DN, 2): ['xy4'], S(DN, 3): ['xy5'],
    S(DN, 4): ['load'],
}


def split3(v):
    hi = v.astype(BF)
    rest = v - hi.astype(F32)
    mid = rest.astype(BF)
    low = (rest - mid.astype(F32)).astype(BF)
    return hi, mid, low


def dot6(a, b, rhs_dim):
    def d(i, j):
        return lax.dot_general(a[i], b[j], (((1,), (rhs_dim,)), ((), ())), preferred_element_type=F32)
    return d(0, 0) + d(1, 0) + d(2, 0) + d(0, 1) + d(1, 1) + d(0, 2)


def table(i, values):
    out = values[0]
    for k, v in enumerate(values):
        if v != values[0]:
            out = jnp.where(i == k, v, out)
    return out


def kernel(x_ref, l_ref, r_ref, w_ref, y_ref, xg, rx, ys, yr, lc_ref,
           t_ref, xbuf, lsp, acc, rbuf,
           ssem, rsem, zsend, zrecv, bsend, brecv, ysend, yrecv, xsem, lsem, csem, psem, bsem, asem, ysem, osem):
    z = lax.axis_index('by')
    me = lax.axis_index('bx')
    core = lax.rem(me, 2)
    cx = lax.rem(me // 2, 2)
    cy = me // 4
    rows, cols = x_ref.shape[0], x_ref.shape[3]
    nf, nb = cols // FB, cols // BT
    half = rows // 2
    hw = cols // 2

    def index(dx, dy, dc):
        return (lax.rem(cy + dy, 2) * 2 + lax.rem(cx + dx, 2)) * 2 + lax.rem(core + dc, 2)

    sib, xn, yn, dn = index(0, 0, 1), index(1, 0, 0), index(0, 1, 0), index(1, 1, 0)
    dev_s, dev_x, dev_y, dev_z = (z, sib), (z, xn), (z, yn), (1 - z, me)

    def remote(src, dst, send, recv, dev):
        return pltpu.make_async_remote_copy(src_ref=src, dst_ref=dst, send_sem=send, recv_sem=recv, device_id=dev,
                                            device_id_type=MESH)

    def piece(ref, k):
        return ref.at[:, :, :, pl.ds(pl.multiple_of(k * FB, FB), FB)]

    def block(kind):
        if kind < 3:
            return xg.at[me]
        if kind == 3:
            return xg.at[yn, pl.ds(0, half)]
        if kind == 4:
            return xg.at[xn, pl.ds(half, half)]
        return xg.at[(xn, yn, dn)[kind - 5]]

    def send(kind, k):
        dst = piece(block(kind), k) if kind or k > 1 else xbuf.at[k, core]
        src = piece(x_ref, k) if kind < 3 else dst
        dev = (dev_s, dev_x, dev_y, dev_x, dev_y, dev_s, dev_s, dev_s)[kind]
        return remote(src, dst, ssem.at[kind, k], rsem.at[kind, k], dev)

    def arrived(kind, k):
        ref = (xg.at[sib], xg.at[xn], xg.at[yn], xg.at[dn, pl.ds(0, half)], xg.at[dn, pl.ds(half, half)],
               xg.at[index(1, 0, 1)], xg.at[index(0, 1, 1)], xg.at[index(1, 1, 1)])[kind]
        part = piece(ref, k) if kind or not isinstance(k, int) else xbuf.at[k, 1 - core]
        remote(part, part, ssem.at[kind, k], rsem.at[kind, k], dev_s).wait_recv()

    def rz(bt):
        rws = pl.ds(bt * BT, BT)
        src = r_ref.at[:, rws, pl.ds(pl.multiple_of((1 - z) * cols + core * hw, 128), hw)]
        dst = rx.at[:, rws, pl.ds(pl.multiple_of(core * hw, 128), hw)]
        return remote(src, dst, zsend.at[bt], zrecv.at[bt], dev_z)

    def rs(bt, c):
        part = rx.at[:, pl.ds(pl.multiple_of(bt * BT, BT), BT), pl.ds(pl.multiple_of(c * hw, 128), hw)]
        return remote(part, part, bsend.at[bt], brecv.at[bt], dev_s)

    def yz(bt):
        return remote(ys.at[bt], yr.at[bt], ysend.at[bt], yrecv.at[bt], dev_z)

    def run(name):
        k = int(name[-1])
        if name[:-1] == 'own':
            send(1, k).start()
            send(2, k).start()
        elif name[:-1] == 'xy':
            arrived(1, k)
            send(4, k).start()
            send(5, k).start()
            arrived(2, k)
            send(3, k).start()
            send(6, k).start()
        elif name[:-1] == 'd':
            arrived(3, k)
            arrived(4, k)
            send(7, k).start()
        elif name[:-1] == 'r':
            rz(k).wait_recv()
            rs(k, core).start()
        elif name[:-1] == 'f':
            flush(0, k).wait()
            yz(k).start()
        elif name[:-1] == 'y':
            yz(k).wait_recv()
            yload(yslot[k], k).start()

    n = len(UNITS)
    xslot, lslot, lmode, rslot = [0] * n, [0] * n, [0] * n, [0] * n
    cnt, prev, ls, seen, rcnt = 0, None, 1, set(), 0
    writes = {}
    for i, u in enumerate(UNITS):
        if u[0] == 's':
            xslot[i] = cnt % 2
            cnt += 1
            if u[1] != prev:
                ls = 1 - ls
                lmode[i] = 2 if u[1] in seen else 1
                if lmode[i] == 1:
                    nxt = next(j for j in range(i + 1, n) if UNITS[j][0] == 's')
                    writes[nxt] = u[1]
                seen.add(u[1])
                prev = u[1]
            lslot[i] = ls
        else:
            rslot[i] = rcnt % 2
            rcnt += 1
    lmode[0] = 0
    at = {i: list(AT.get(u, ())) for i, u in enumerate(UNITS)}
    mid = {i: list(MID.get(u, ())) for i, u in enumerate(UNITS)}
    mixk = [0 for u in UNITS]
    mixa = [MIX_AFTER.get(u, -1) + 1 for u in UNITS]
    init = [int(u[0] == 's' and all(v[0] != 's' or v[2] != u[2] for v in UNITS[:i])) for i, u in enumerate(UNITS)]
    sums = [i for i, u in enumerate(UNITS) if u[0] == 't']
    aslot, first, last = [0] * n, [0] * n, [0] * n
    order, yslot = [], {}
    for i in sums:
        tile = UNITS[i][1:3]
        if tile not in order:
            order.append(tile)
            first[i] = 1
        aslot[i] = order.index(tile) % 2
        yslot[tile[1]] = 1 - aslot[i]
        if all(UNITS[j][1:3] != tile for j in sums if j > i):
            last[i] = 1
            if tile[0] == 0:
                at[i + (1 if tile[1] == 0 else 2)].append('f%d' % tile[1])
            else:
                if tile[1] < nb - 1:
                    at[i].append('y%d' % tile[1])
    is_t = [int(u[0] == 't') for u in UNITS]
    arg = [[u[j] if len(u) > j else 0 for u in UNITS] for j in range(1, 4)]
    late = [int(u in LATE) for u in UNITS]

    def chip(rel):
        return lax.rem(cy + rel // 2, 2) * 2 + lax.rem(cx + lax.rem(rel, 2), 2)

    def xcopies(slot, rel, k):
        c = chip(rel) * 2
        return (pltpu.make_async_copy(piece(x_ref, k), xbuf.at[slot, core], xsem.at[slot, 0]),
                pltpu.make_async_copy(piece(xg.at[c + core], k), xbuf.at[slot, core], xsem.at[slot, 0]),
                pltpu.make_async_copy(piece(xg.at[c + 1 - core], k), xbuf.at[slot, 1 - core], xsem.at[slot, 1]))

    def xstart(slot, rel, k):
        rel = jnp.int32(rel)
        own, far, sibling = xcopies(slot, rel, k)

        @pl.when(rel == OWN)
        def _():
            own.start()

        @pl.when(rel != OWN)
        def _():
            far.start()
        for r, kind in ((OWN, 0), (XN, 5), (YN, 6), (DN, 7)):
            @pl.when(rel == r)
            def _():
                arrived(kind, k)
        sibling.start()

    def lcopies(rel, what):
        base = chip(rel) * 2 * rows
        for j, (dst, off, width) in enumerate(((acc.at[0, pl.ds(0, 3)], 0, BT), (acc.at[1, pl.ds(0, 3), :, pl.ds(0, FB)], BT, FB))):
            src = l_ref.at[:, :, pl.ds(pl.multiple_of(base + off, 128), width)]
            getattr(pltpu.make_async_copy(src, dst, lsem.at[j]), what)()

    def cload(slot, rel):
        return pltpu.make_async_copy(lc_ref.at[rel], lsp.at[slot], csem)

    def cstore(slot, rel):
        return pltpu.make_async_copy(lsp.at[slot], lc_ref.at[rel], psem)

    def rcopies(slot, bt, pair):
        rws = pl.ds(pl.multiple_of(bt * BT, BT), BT)
        return (pltpu.make_async_copy(rx.at[:, rws, pl.ds(pl.multiple_of(pair * 512, 512), 512)], rbuf.at[slot], bsem.at[slot]),
                pltpu.make_async_copy(r_ref.at[:, rws, pl.ds(pl.multiple_of(z * cols + pair * 512, 512), 512)], rbuf.at[slot],
                                      bsem.at[slot]))

    def flush(slot, bt):
        return pltpu.make_async_copy(acc.at[slot], ys.at[bt], asem)

    def yload(slot, bt):
        return pltpu.make_async_copy(yr.at[bt], acc.at[slot], ysem)

    def yout(bt, h):
        return pltpu.make_async_copy(xbuf.at[1, h], y_ref.at[:, :, :, pl.ds(pl.multiple_of(bt * BT + h * FB, FB), FB)],
                                     osem.at[h])

    def lsplit(slot):
        def body(j, carry):
            sl = pl.ds(pl.multiple_of(j * 16, 16), 16)
            for u in range(3):
                for j, (off, width) in enumerate(((0, BT), (BT, FB))):
                    for part, v in enumerate(split3(acc[j, u, sl, :width])):
                        lsp[slot, part, u, sl, off:off + width] = v
            return carry
        lax.fori_loop(0, rows // 16, body, 0, unroll=2)

    lcopies(OWN, 'start')
    for k in range(2):
        xcopies(k, OWN, k)[0].start()
    barrier = pltpu.get_barrier_semaphore()
    for dev in (dev_s, dev_x, dev_y, dev_z):
        pl.semaphore_signal(barrier, inc=1, device_id=dev, device_id_type=MESH)
    pl.semaphore_wait(barrier, 4)
    for k in range(2):
        send(0, k).start()
    run('own0')
    for bt in range(nb):
        rz(bt).start()
    run('own1')
    for k in range(2, nf):
        send(0, k).start()
    lcopies(OWN, 'wait')
    lsplit(0)
    cstore(0, OWN).start()
    xcopies(0, OWN, 0)[0].wait()
    arrived(0, 0)

    def mix8(k, row):
        w = {(u, s, p, v): w_ref[u, s, p, v] for u in range(3) for s in range(2) for p in range(2) for v in range(3)}

        def wt(u, s, p, v):
            return w[u, s, p, v]

        for h in range(FB // 128):
            sl = (pl.ds(pl.multiple_of(row, 8), 8), slice(h * 128, (h + 1) * 128))
            t = [t_ref[(k, c) + sl] for c in range(12)]
            md = {}
            for s in range(2):
                for v in range(3):
                    for q in range(2):
                        terms = [t[(u * 2 + p) * 2 + q] * wt(u, s, p, v) for u in range(3) for p in range(2)]
                        md[s, v, q] = functools.reduce(lambda m, o: m + o, terms)
            for s in range(2):
                for tt in range(2):
                    for r in range(3):
                        terms = [md[s, v, q] * wt(v, tt, q, r) for v in range(3) for q in range(2)]
                        t_ref[(k, (s * 2 + tt) * 3 + r) + sl] = functools.reduce(lambda m, o: m + o, terms)

    writes = set(writes)
    fields = [(is_t, 2), (arg[0], 4), (arg[1], 8), (arg[2], 4), (xslot, 2), (lslot, 2), (lmode, 4), (rslot, 2), (aslot, 2),
              (first, 2), (last, 2), (late, 2), ([int(bool(at[i]) or i in writes) for i in range(n)], 2),
              ([int(bool(mid[i])) for i in range(n)], 2), (mixk, 8), (mixa, 8), (init, 2)]
    codes = []
    for i in range(n):
        code = 0
        for values, base in reversed(fields):
            code = code * base + values[i]
        codes.append(code)

    def decode(code):
        out = []
        for _, base in fields:
            out.append(jnp.bitwise_and(code, base - 1))
            code = jnp.right_shift(code, base.bit_length() - 1)
        return out

    def unit(i, code):
        kind, a0, a1, a2, xs_, ls_, lm_, rs_, as_, first_, last_, late_, ev_, evm_, mixk_, mixa_, init_ = decode(code)
        code1 = table(i, codes[1:] + [0])
        kind1, b0, b1, b2, xs1, ls1, lm1, rs1, _, first1, _, late1 = decode(code1)[:12]

        @pl.when(ev_ == 1)
        def _():
            for j in range(n):
                if at[j] or j in writes:
                    @pl.when(i == j)
                    def _():
                        if j in writes:
                            cstore(0, 0).wait()
                        for name in at[j]:
                            run(name)

        @pl.when(kind == 0)
        def _():
            @pl.when(i == 1)
            def _():
                xcopies(1, OWN, 1)[0].wait()
                arrived(0, 1)

            @pl.when(i > 1)
            def _():
                _, far, sibling = xcopies(xs_, a0, a1)
                far.wait()
                sibling.wait()

            @pl.when(lm_ == 1)
            def _():
                lcopies(a0, 'wait')
                lsplit(ls_)
                cstore(ls_, a0).start()

            @pl.when(lm_ == 2)
            def _():
                cload(ls_, a0).wait()

        @pl.when(kind == 1)
        def _():
            rcopies(rs_, a1, a2)[0].wait()

        def ahead():
            @pl.when(kind1 == 0)
            def _():
                @pl.when(jnp.logical_and(late1 == 0, i > 0))
                def _():
                    xstart(xs1, b0, b1)

                @pl.when(lm1 == 1)
                def _():
                    lcopies(b0, 'start')

                @pl.when(lm1 == 2)
                def _():
                    cload(ls1, b0).start()

            @pl.when(kind1 == 1)
            def _():
                @pl.when(b0 == 0)
                def _():
                    @pl.when(first1 == 1)
                    def _():
                        rs(b1, 1 - core).wait_recv()
                    rcopies(rs1, b1, b2)[0].start()

                @pl.when(b0 == 1)
                def _():
                    rcopies(rs1, b1, b2)[1].start()

        @pl.when(i + 1 < n)
        def _():
            ahead()

        @pl.when(kind == 0)
        def _():
            for p in range(2):
                for q in range(2):
                    xs = jnp.concatenate([xbuf[xs_, 0, :, p, q, :], xbuf[xs_, 1, :, p, q, :]], axis=0)
                    xparts = split3(xs)
                    for u in range(3):
                        idx = (u * 2 + p) * 2 + q
                        old = jnp.where(init_ == 1, 0.0, t_ref[a1, idx])
                        t_ref[a1, idx] = dot6([lsp[ls_, j, u] for j in range(3)], xparts, 0) + old

        @pl.when(evm_ == 1)
        def _():
            for j in range(n):
                if mid[j]:
                    @pl.when(i == j)
                    def _():
                        for name in mid[j]:
                            if name == 'load':
                                xstart(xslot[j + 1], *UNITS[j + 1][1:])
                            else:
                                run(name)

        @pl.when(mixa_ > 0)
        def _():
            def body(j, carry):
                mix8(mixa_ - 1, j * 8)
                return carry
            lax.fori_loop(0, rows // 16, body, 0, unroll=4)
            for j in range(n):
                if UNITS[j] in HALFWAY:
                    @pl.when(i == j)
                    def _():
                        xstart(xslot[j + 1], *UNITS[j + 1][1:])
            lax.fori_loop(rows // 16, rows // 8, body, 0, unroll=4)

        @pl.when(kind == 1)
        def _():
            rparts = [[split3(rbuf[rs_, r, :, f * FB:(f + 1) * FB]) for f in range(2)] for r in range(3)]
            for st in range(4):
                tot = jnp.where(first_ == 1, 0.0, acc[as_, st])
                for r in range(3):
                    for f in range(2):
                        tot = dot6(split3(t_ref[a2 * 2 + f, st * 3 + r]), rparts[r][f], 1) + tot
                acc[as_, st] = tot

            @pl.when(last_ == 1)
            def _():
                @pl.when(a0 == 0)
                def _():
                    flush(as_, a1).start()

                @pl.when(a0 == 1)
                def _():
                    @pl.when(i == n - 1)
                    def _():
                        run('y%d' % (nb - 1))

                    @pl.when(a1 > 0)
                    def _():
                        for h in range(2):
                            yout(a1 - 1, h).wait()
                    yload(1 - as_, a1).wait()
                    for h in range(2):
                        for s in range(2):
                            for tt in range(2):
                                st = s * 2 + tt
                                part = acc[1 - as_, st, :, h * FB:(h + 1) * FB]
                                xbuf[1, h, :, s, tt, :] = acc[as_, st, :, h * FB:(h + 1) * FB] + part
                        yout(a1, h).start()
        return code1

    lax.fori_loop(0, n, unit, jnp.int32(codes[0]))
    for h in range(2):
        yout(nb - 1, h).wait()
    for bt in range(nb):
        rz(bt).wait_send()
        rs(bt, core).wait_send()
        yz(bt).wait_send()
    for k in range(nf):
        for kd in range(8):
            send(kd, k).wait_send()


def apply_local(x, left, w, right):
    rows, cols = x.shape[0], x.shape[3]
    lt = jnp.transpose(left, (1, 0, 2))
    rt = jnp.transpose(right, (1, 0, 2))
    nf, nb = cols // FB, cols // BT
    hbm = pl.BlockSpec(memory_space=pltpu.HBM)
    shape = jax.ShapeDtypeStruct
    dma = pltpu.SemaphoreType.DMA
    tiles = shape((nb, 4, rows, BT), F32)
    out = pl.pallas_call(
        kernel,
        out_shape=[shape(x.shape, F32), shape((8,) + x.shape, F32), shape((3, cols, cols), F32), tiles, tiles,
                   shape((4, 3, 3, rows, 2 * rows), BF)],
        in_specs=[hbm, hbm, hbm, pl.BlockSpec(memory_space=pltpu.SMEM)],
        out_specs=[hbm] * 6,
        scratch_shapes=[
            pltpu.VMEM((nf, 12, rows, FB), F32),
            pltpu.VMEM((2, 2, rows, 2, 2, FB), F32),
            pltpu.VMEM((2, 3, 3, rows, 2 * rows), BF),
            pltpu.VMEM((2, 4, rows, BT), F32),
            pltpu.VMEM((2, 3, BT, 512), F32),
            dma((8, nf)), dma((8, nf)), dma((nb,)), dma((nb,)), dma((nb,)), dma((nb,)), dma((nb,)), dma((nb,)),
            dma((2, 2)), dma((2,)), dma, dma, dma((2,)), dma, dma, dma((2,)),
        ],
        compiler_params=pltpu.CompilerParams(collective_id=0, has_side_effects=True, vmem_limit_bytes=67043328),
        name="heff",
    )(x, lt, rt, w)
    return out[0]


def solution(mesh):
    return jax.shard_map(apply_local, mesh=mesh,
                         in_specs=(P('bx', None, None, 'by'), P('bx', None, None), P(), P('by', None, None)),
                         out_specs=P('bx', None, None, 'by'), check_vma=False)
```
